32 devices in a mesh: gx: 4 (over x, core), gy: 8 (over z, y).
Axes of the slice: x: 2, y: 2, z: 4, core: 2. Of those that a mesh axis runs over, the one named last changes fastest.
Arguments:
- emission: bfloat16 [98304, 128], P(('gx', 'gy')), may hold values from -6 to 6
- reflectance: float32 [98304], P(('gx', 'gy')), may hold values from 0.3 to 0.9
- link_blocks: bfloat16 [4608, 256, 256], P(('gx', 'gy')), may hold values from -0.109375 to 0.109375
- link_source: int32 [4608], P(('gx', 'gy')), may hold values from 0 to 11
- link_target: int32 [4608, 1], P(('gx', 'gy')), may hold values from 0 to 31, as said below
- link_slot: int32 [4608], P(('gx', 'gy')), may hold values from 0 to 11
- sensor_cell: int32 [16384, 8], P(('gx', 'gy')), may hold values from 0 to 9215
- sensor_weight: float32 [16384, 8], P(('gx', 'gy')), may hold values from 0 to 0.25
Outputs:
- radiosity: float32 [98304, 128], P(('gx', 'gy'))
- sensor_values: float32 [16384, 128], P(('gx', 'gy'))
The draws below stay inside these ranges and needn't reach their ends.
Inputs may be any that keep to these rules, and one draw needn't show every extreme that they name: `link_target`: the owner of each block is the device that holds it or one of that device's neighbours (i +- 1, j) or (i, j +- 1) inside the grid of devices, without wrapping. Among the 144 blocks of one device at most 9 name any one neighbour, and some neighbour is named exactly 9 times.
All inputs are finite; a program needn't handle non-finite values.
Results may differ from the reference program's by a relative error of at most 0.0039.
Values may be sent and summed in bfloat16 or wider, within the bound.
A program may use at most 128 MiB of HBM per device.

```python
import jax
import jax.numpy as jnp
from jax import lax

P_SIZE = 256
S = 128
CL_DEV = 12
LINKS = 12
SWEEPS = 2
SENS_DEV = 512
TAPS = 8
CLUSTERS = 384
LINK_DEV = 144
LINKS_ALL = 4608
CAP = 9
SENSORS = 16384
N_GX = 4
N_GY = 8


def draw_link_target(key, part):
    devices = N_GX * N_GY
    index = jnp.arange(devices, dtype=jnp.int32)
    row = index // N_GY
    col = index % N_GY
    exists = jnp.stack([row + 1 < N_GX, row >= 1, col + 1 < N_GY, col >= 1], axis=1).astype(jnp.int32)
    owners = jnp.stack([index + N_GY, index - N_GY, index + 1, index - 1, index], axis=1)
    first_key, second_key, third_key = jax.random.split(jax.random.fold_in(key, 11), 3)
    lowest = max(1, CAP // 2)
    counts = jax.random.randint(first_key, (devices, 4), lowest, CAP + 1).astype(jnp.int32) * exists
    start = jax.random.randint(second_key, (devices,), 0, 4).astype(jnp.int32)
    order = (start[:, None] + jnp.arange(4, dtype=jnp.int32)[None, :]) % 4
    exists_turned = jnp.take_along_axis(exists, order, axis=1)
    first = jnp.argmax(exists_turned, axis=1).astype(jnp.int32)
    picked = jnp.take_along_axis(order, first[:, None], axis=1)[:, 0]
    counts = jnp.where(jnp.arange(4, dtype=jnp.int32)[None, :] == picked[:, None], CAP, counts)
    edges = jnp.cumsum(counts, axis=1)
    position = jnp.arange(LINK_DEV, dtype=jnp.int32)
    label = jnp.sum((position[None, :, None] >= edges[:, None, :]).astype(jnp.int32), axis=2)
    target = jnp.take_along_axis(owners, label, axis=1)
    scores = jax.random.randint(third_key, (devices, LINK_DEV), 0, 1 << 20).astype(jnp.int32) * LINK_DEV + position[None, :]
    shuffle = jnp.argsort(scores, axis=1)
    target = jnp.take_along_axis(target, shuffle, axis=1)
    return target.reshape(devices * LINK_DEV, 1).astype(jnp.int32)


def place_ends(drawn, key, smallest, high):
    longest = drawn.shape.index(max(drawn.shape))
    spots = []
    for shift in (0, 1):
        where = [jax.random.randint(jax.random.fold_in(key, axis), (), 0, length) for axis, length in enumerate(drawn.shape)]
        where[longest] = (where[longest] + shift) % drawn.shape[longest]
        spots.append(tuple(where))
    return drawn.at[spots[0]].set(smallest).at[spots[1]].set(high)


def shard_levels(key, extent, cuts, smallest, largest):
    factor_of, own = 1.0, jax.random.fold_in(key, 6)
    for dim, shards_of in cuts:
        heights = jnp.exp(jax.random.uniform(jax.random.fold_in(own, dim), (shards_of,), jnp.float32, smallest / len(cuts), largest / len(cuts)))
        factor_of = factor_of * jnp.repeat(heights, extent[dim] // shards_of).reshape([-1 if axis == dim else 1 for axis in range(len(extent))])
    return factor_of


def centred(key, dims, spread, bound, shards=(), kind=jnp.bfloat16):
    gain = shard_levels(key, dims, shards, -0.22, 0.18) if shards else 1.0
    array = jax.random.normal(key, dims, jnp.float32) * spread * gain
    return jnp.minimum(jnp.maximum(array, -bound), bound).astype(kind)


def setup_inputs(seed: int = 0) -> dict:
    arg_keys = jax.random.split(jax.random.key(seed), 9)
    emission = centred(arg_keys[0], (CLUSTERS * P_SIZE, S), 1.0, 6.0, ((0, 32),))
    reflectance = jnp.clip(0.3 + 0.59999996 * jax.random.uniform(arg_keys[1], (CLUSTERS * P_SIZE,), jnp.float32) ** shard_levels(arg_keys[1], (CLUSTERS * P_SIZE,), ((0, 32),), -0.2, 0.2), 0.3, 0.9)
    link_blocks = centred(arg_keys[2], (LINKS_ALL, P_SIZE, P_SIZE), (P_SIZE * LINKS) ** -0.5, 0.109375, ((0, 32),))
    link_source = place_ends(jax.random.randint(arg_keys[3], (LINKS_ALL,), 0, CL_DEV), jax.random.fold_in(arg_keys[3], 1), 0, CL_DEV - 1).astype(jnp.int32)
    link_target = draw_link_target(jax.random.fold_in(arg_keys[8], 71), 0)
    link_slot = place_ends(jax.random.randint(arg_keys[5], (LINKS_ALL,), 0, CL_DEV), jax.random.fold_in(arg_keys[5], 1), 0, CL_DEV - 1).astype(jnp.int32)
    sensor_cell = place_ends(jax.random.randint(arg_keys[6], (SENSORS, TAPS), 0, 3 * CL_DEV * P_SIZE), jax.random.fold_in(arg_keys[6], 1), 0, (3 * CL_DEV * P_SIZE) - 1).astype(jnp.int32)
    sensor_weight = jnp.clip(0.25 * jax.random.uniform(arg_keys[7], (SENSORS, TAPS), jnp.float32) ** shard_levels(arg_keys[7], (SENSORS, TAPS), ((0, 32),), -0.2, 0.2), 0.0, 0.25)
    return {"emission": emission, "reflectance": reflectance, "link_blocks": link_blocks, "link_source": link_source, "link_target": link_target, "link_slot": link_slot, "sensor_cell": sensor_cell, "sensor_weight": sensor_weight}


def reference(emission, reflectance, link_blocks, link_source, link_target, link_slot, sensor_cell, sensor_weight):
    devices = N_GX * N_GY
    clusters = CL_DEV * devices
    base = emission.astype(jnp.float32)
    blocks = link_blocks.reshape(devices, LINK_DEV, P_SIZE, P_SIZE)
    offsets = (CL_DEV * jnp.arange(devices, dtype=jnp.int32))[:, None]
    sources = (link_source.reshape(devices, LINK_DEV) + offsets).astype(jnp.int32)
    targets = (link_target[:, 0] * CL_DEV + link_slot).reshape(devices, LINK_DEV).astype(jnp.int32)
    radiosity = base
    for sweep in range(SWEEPS):
        rounded = radiosity.astype(jnp.bfloat16)
        rounded = lax.optimization_barrier(rounded).astype(jnp.float32).reshape(clusters, P_SIZE, S)

        def step(incoming, item):
            block, source, target = item
            term = jnp.einsum("lpq,lqs->lps", block.astype(jnp.float32), rounded[source],
                              precision=lax.Precision.HIGHEST).astype(jnp.bfloat16)
            term = lax.optimization_barrier(term).astype(jnp.float32)
            return incoming.at[target].add(term), None

        incoming, _ = lax.scan(step, jnp.zeros((clusters, P_SIZE, S), jnp.float32), (blocks, sources, targets))
        radiosity = base + reflectance[:, None] * incoming.reshape(clusters * P_SIZE, S)
    rows = CL_DEV * P_SIZE
    final = radiosity.astype(jnp.bfloat16).reshape(N_GX, N_GY, rows, S)
    padded = jnp.pad(final, ((0, 0), (1, 1), (0, 0), (0, 0))).reshape(-1, S)
    device_of = (jnp.arange(SENS_DEV * devices, dtype=jnp.int32) // SENS_DEV).astype(jnp.int32)
    row_index = (device_of // N_GY).astype(jnp.int32)
    col_index = (device_of % N_GY).astype(jnp.int32)
    which = sensor_cell // rows
    within = sensor_cell % rows
    flat = ((row_index[:, None] * (N_GY + 2) + col_index[:, None] + which) * rows + within).astype(jnp.int32)
    sensor_values = jnp.zeros((SENS_DEV * devices, S), jnp.float32)
    for tap in range(TAPS):
        sensor_values = sensor_values + sensor_weight[:, tap][:, None] * padded[flat[:, tap]].astype(jnp.float32)
    return radiosity, sensor_values
```

```python
import functools

import jax
import jax.numpy as jnp
from jax import lax
from jax.experimental import pallas as pl
from jax.experimental.pallas import tpu as pltpu
from jax.sharding import PartitionSpec as P

P_SIZE = 256
S = 128
SWEEPS = 2
TAPS = 8
MESH = pl.DeviceIdType.MESH
MOVES = (("gy", 1), ("gy", -1), ("gx", 1), ("gx", -1))


def ceil_to(n, m):
    return -(-n // m) * m


def divisor_up_to(n, most):
    return max(d for d in range(1, most + 1) if n % d == 0)


def turned(row, size):
    return jnp.transpose(jnp.broadcast_to(row, (size, row.shape[1])))


def make_tables(target, slot, source, me, cols, dims):
    links, clusters, cap, per_group, groups, lanes = (
        dims["links"], dims["clusters"], dims["cap"], dims["per_group"], dims["groups"], dims["lanes"],
    )
    lane = lax.broadcasted_iota(jnp.int32, (1, lanes), 1)
    ways = 4 * cap
    away = target - me
    group = jnp.where(
        away == 0, 4, jnp.where(away == cols, 2, jnp.where(away == -cols, 3, jnp.where(away == 1, 0, 1)))
    )
    group = jnp.where(lane < links, group, 5)
    base = group * (clusters * lanes)
    key = base + slot * lanes + lane
    key_m = turned(key, lanes)
    rank = jnp.sum(jnp.where((key_m < key) & (key_m >= base), 1, 0), axis=0, keepdims=True)
    place = jnp.where(group == 4, ways + rank, group * cap + rank)
    place = jnp.where(lane < links, place, -1)
    code = lane + lanes * (source + 64 * (slot + 64))
    place_m, code_m = turned(place, lanes), turned(code, lanes)
    wide = lax.broadcasted_iota(jnp.int32, (lanes, lanes), 1)
    found = jnp.sum(jnp.where(place_m == wide, code_m, 0), axis=0, keepdims=True)
    block = found & (lanes - 1)
    rest = found >> (lanes.bit_length() - 1)
    from_cluster = rest & 63
    into = jnp.where(rest >= 4096, (rest >> 6) & 63, -1)
    starts = [w * cap for w in range(4)] + [ways + g * per_group for g in range(groups)]
    ends = starts[1:] + [ways + groups * per_group]
    keep = into == pltpu.roll(jnp.broadcast_to(into, (8, lanes)), 1, 1)[0:1]
    for start in starts:
        keep = keep & (lane != start)
    keep = jnp.where(keep & (into >= 0), 1, 0)
    into_m = turned(into, lanes)
    order = lax.broadcasted_iota(jnp.int32, (lanes, lanes), 0)
    first = jnp.zeros((1, lanes), jnp.int32)
    end = jnp.zeros((1, lanes), jnp.int32)
    cluster = jnp.full((1, lanes), -2, jnp.int32)
    for g in range(4 + groups):
        inside = (lane >= g * clusters) & (lane < (g + 1) * clusters)
        first = jnp.where(inside, starts[g], first)
        end = jnp.where(inside, ends[g], end)
        cluster = jnp.where(inside, lane - g * clusters, cluster)
    hit = (into_m == cluster) & (order >= first) & (order < end)
    last = jnp.max(jnp.where(hit, order - first + 1, 0), axis=0, keepdims=True)
    row = lax.broadcasted_iota(jnp.int32, (8, lanes), 0)
    return jnp.where(row == 0, block, jnp.where(row == 1, from_cluster, jnp.where(row == 2, keep, last)))


def fused_kernel(
    target, slot, source, cells, weights, reflect, emission_hbm, blocks_hbm,
    rad_hbm, values,
    blocks, emission, rounded, rad, refl, acc, running, arrived, sends, recvs, item_cell, item_weight, from_cell,
    from_weight, sensor_w, final_t, sum_send, sum_recv, sum_own, table, table_in, table_s, table_in_s,
    load_sem, table_sem, small_send, small_recv, term_send, term_recv, sum_ssem, sum_rsem,
    *, dims,
):
    clusters, cap, per_group, groups = dims["clusters"], dims["cap"], dims["per_group"], dims["groups"]
    unroll, chunks, loads, sensors = dims["unroll"], dims["chunks"], dims["loads"], dims["sensors"]
    rows, links, lanes = dims["rows"], dims["links"], dims["lanes"]
    ways = 4 * cap
    per_chunk = cap // chunks
    wide = dims["wide"]
    pieces = sensors // wide
    i, j = lax.axis_index("gx"), lax.axis_index("gy")
    n_gx, n_gy = lax.axis_size("gx"), lax.axis_size("gy")
    me = i * n_gy + j

    def there(way, back=False):
        axis, step = MOVES[way]
        step = -step if back else step
        at = (j if axis == "gy" else i) + step
        inside = (at >= 0) & (at < (n_gy if axis == "gy" else n_gx))
        return inside, ((i, at) if axis == "gy" else (at, j))

    def remote(src, dst, send, recv, way):
        return pltpu.make_async_remote_copy(
            src_ref=src, dst_ref=dst, send_sem=send, recv_sem=recv, device_id=there(way)[1], device_id_type=MESH
        )

    def if_to(way, act):
        pl.when(there(way)[0])(act)

    def if_from(way, act):
        pl.when(there(way, back=True)[0])(act)

    share = links // loads
    reads = [
        pltpu.make_async_copy(emission_hbm, emission, load_sem.at[loads]),
        pltpu.make_async_copy(emission_hbm, rounded, load_sem.at[loads + 1]),
    ] + [
        pltpu.make_async_copy(blocks_hbm.at[pl.ds(n * share, share)], blocks.at[pl.ds(n * share, share)], load_sem.at[n])
        for n in range(loads)
    ]
    for read in reads:
        read.start()

    barrier = pltpu.get_barrier_semaphore()
    for way in range(4):
        if_to(way, lambda way=way: pl.semaphore_signal(barrier, 1, device_id=there(way)[1], device_id_type=MESH))

    table[...] = make_tables(target[...], slot[...], source[...], me, n_gy, dims)
    table_copy = pltpu.make_async_copy(table, table_s, table_sem.at[0])
    table_copy.start()

    pl.semaphore_wait(barrier, sum(jnp.where(there(way)[0], 1, 0) for way in range(4)))

    def table_send(way):
        return remote(table, table_in.at[way], small_send.at[0, way], small_recv.at[0, way], way)

    def cell_send(way):
        return remote(cells, from_cell.at[way], small_send.at[1, way], small_recv.at[1, way], way)

    def weight_send(way):
        return remote(weights, from_weight.at[way], small_send.at[2, way], small_recv.at[2, way], way)

    for way in range(4):
        if_to(way, lambda way=way: table_send(way).start())
    for way in range(2):
        if_to(way, lambda way=way: cell_send(way).start())
        if_to(way, lambda way=way: weight_send(way).start())

    def spread(t, carry):
        at = pl.ds(pl.multiple_of(t * 128, 128), 128)
        refl[at, :] = turned(reflect[pl.ds(t, 1), :], 128)
        return carry

    lax.fori_loop(0, rows // 128, spread, 0)

    running[0] = jnp.zeros((P_SIZE, S), jnp.float32)
    for way in range(4):
        arrived[way, 0] = jnp.zeros((P_SIZE, S), jnp.float32)

        @pl.when(jnp.logical_not(there(way, back=True)[0]))
        def _(way=way):
            table_in[way] = jnp.zeros(table_in.shape[1:], jnp.int32)
            if way < 2:
                from_cell[way] = jnp.full(from_cell.shape[1:], -1, jnp.int32)
                from_weight[way] = jnp.zeros(from_weight.shape[1:], jnp.float32)
                sum_recv[way] = jnp.zeros(sum_recv.shape[1:], sum_recv.dtype)

    for way in range(4):
        if_from(way, lambda way=way: table_send(way).wait_recv())
    table_in_copy = pltpu.make_async_copy(table_in, table_in_s, table_sem.at[1])
    table_in_copy.start()
    for way in range(2):
        if_from(way, lambda way=way: cell_send(way).wait_recv())
        if_from(way, lambda way=way: weight_send(way).wait_recv())

    for part in range(3):
        cell = cells[...] if part == 2 else from_cell[part]
        weight = weights[...] if part == 2 else from_weight[part]
        total = weight
        for turn in range(1, TAPS):
            total = total + jnp.where(
                cell == pltpu.roll(cell, turn, 0), pltpu.roll(weight, turn, 0), jnp.zeros_like(weight)
            )
        item_cell[part] = cell - (2 * rows, 0, rows)[part]
        item_weight[part] = total

    table_copy.wait()
    table_in_copy.wait()
    for read in reads:
        read.wait()

    def product(q):
        return jnp.dot(blocks[table_s[0, q]], rounded[table_s[1, q]], preferred_element_type=jnp.float32)

    def term_copy(sweep, way, chunk):
        at = pl.ds(way * cap + chunk * per_chunk, per_chunk)
        return remote(
            sends.at[sweep, at], recvs.at[sweep, at], term_send.at[sweep, way, chunk], term_recv.at[sweep, way, chunk], way
        )

    def send_terms(sweep, pair):
        def body(chunk, carry):
            for way in pair:
                for r in range(per_chunk):
                    q = way * cap + chunk * per_chunk + r
                    sends[sweep, q] = product(q).astype(jnp.bfloat16)
            for way in pair:
                if_to(way, lambda way=way: term_copy(sweep, way, chunk).start())
            return carry

        lax.fori_loop(0, chunks, body, 0)

    def stay():
        def group(g, carry):
            def body(t, carry):
                at = t * unroll
                for u in range(unroll):
                    q = ways + g * per_group + at + u
                    held = jnp.where(table_s[2, q] != 0, running[at + u], 0.0)
                    running[at + u + 1] = product(q) + held
                return carry

            lax.fori_loop(0, per_group // unroll, body, 0)

            def into(c, carry):
                acc[c] += running[table_s[3, (4 + g) * clusters + c]]
                return carry

            lax.fori_loop(0, clusters, into, 0)
            return carry

        lax.fori_loop(0, groups, group, 0)

    def receive(sweep, pair):
        def body(chunk, carry):
            for way in pair:
                def scan(way=way):
                    term_copy(sweep, way, chunk).wait_recv()
                    for r in range(per_chunk):
                        n = chunk * per_chunk + r
                        held = jnp.where(table_in_s[way, 2, way * cap + n] != 0, arrived[way, n], 0.0)
                        arrived[way, n + 1] = recvs[sweep, way * cap + n].astype(jnp.float32) + held

                if_from(way, scan)
            return carry

        lax.fori_loop(0, chunks, body, 0)

    def taken(way, c):
        return arrived[way, table_in_s[way, 3, way * clusters + c]]

    tile = 16
    block_rows = 8 * tile
    columns = 3 * sensors // 128
    per_wide = wide // 128

    def sensor_weights(first, count):
        near = lax.broadcasted_iota(jnp.int32, (tile, 128), 0)

        def column(n, carry):
            part = n // (sensors // 128)
            at = pl.ds(pl.multiple_of((n - part * (sensors // 128)) * 128, 128), 128)
            cell = [
                jnp.broadcast_to(item_cell[part, k : k + 1, at], (tile, 128)).astype(jnp.int16) for k in range(TAPS)
            ]
            weight = [
                jnp.broadcast_to(item_weight[part, k : k + 1, at], (tile, 128)).astype(jnp.bfloat16)
                for k in range(TAPS)
            ]
            to = pl.ds(pl.multiple_of((n - (n // per_wide) * per_wide) * 128, 128), 128)

            def body(t, carry):
                for h in range(8):
                    row = pl.multiple_of(t * block_rows + h * tile, tile)
                    here = (near + row).astype(jnp.int16)
                    total = jnp.zeros((tile, 128), jnp.bfloat16)
                    for k in range(TAPS):
                        total = jnp.where(cell[k] == here, weight[k], total)
                    sensor_w[n // per_wide, pl.ds(row, tile), to] = total
                return carry

            lax.fori_loop(0, rows // block_rows, body, 0)
            return carry

        lax.fori_loop(first, first + count, column, 0)

    def sweep_body(sweep, carry):
        send_terms(sweep, (0, 1))
        send_terms(sweep, (2, 3))
        acc[...] = jnp.zeros(acc.shape, jnp.float32)
        stay()
        sensor_weights(sweep * (columns // SWEEPS), columns // SWEEPS)
        receive(sweep, (2, 3))

        def add_x(c, carry):
            acc[c] += taken(2, c) + taken(3, c)
            return carry

        lax.fori_loop(0, clusters, add_x, 0)
        receive(sweep, (0, 1))

        def finish(c, carry):
            at = pl.ds(pl.multiple_of(c * P_SIZE, P_SIZE), P_SIZE)
            incoming = acc[c] + taken(0, c) + taken(1, c)
            value = emission[c].astype(jnp.float32) + refl[at, :] * incoming
            rounded[c] = value.astype(jnp.bfloat16)
            rad[c] = value
            final_t[:, at] = jnp.transpose(value).astype(jnp.bfloat16)
            return carry

        lax.fori_loop(0, clusters, finish, 0)
        return carry

    lax.fori_loop(0, SWEEPS, sweep_body, 0)

    write = pltpu.make_async_copy(rad, rad_hbm, load_sem.at[0])
    write.start()

    def sum_copy(way, piece):
        return remote(
            sum_send.at[way, piece], sum_recv.at[way, piece], sum_ssem.at[way, piece], sum_rsem.at[way, piece], way
        )

    def sums(part, piece):
        return jnp.dot(final_t[...], sensor_w[part * pieces + piece], preferred_element_type=jnp.float32)

    for piece in range(pieces):
        for part in range(2):
            way = 1 - part
            sum_send[way, piece] = sums(part, piece).astype(jnp.bfloat16)
            if_to(way, lambda: sum_copy(way, piece).start())
    for piece in range(pieces):
        sum_own[piece] = sums(2, piece)
    for piece in range(pieces):
        for way in range(2):
            if_from(way, lambda: sum_copy(way, piece).wait_recv())
        total = sum_own[piece] + sum_recv[0, piece].astype(jnp.float32) + sum_recv[1, piece].astype(jnp.float32)
        values[piece * wide : (piece + 1) * wide, :] = jnp.transpose(total)

    write.wait()
    for way in range(4):
        if_to(way, lambda way=way: table_send(way).wait_send())
        for sweep in range(SWEEPS):
            for chunk in range(chunks):
                if_to(way, lambda: term_copy(sweep, way, chunk).wait_send())
    for way in range(2):
        if_to(way, lambda way=way: cell_send(way).wait_send())
        if_to(way, lambda way=way: weight_send(way).wait_send())
        for piece in range(pieces):
            if_to(way, lambda: sum_copy(way, piece).wait_send())


def per_device(
    emission,
    reflectance,
    link_blocks,
    link_source,
    link_target,
    link_slot,
    sensor_cell,
    sensor_weight,
):
    links = link_blocks.shape[0]
    rows = emission.shape[0]
    clusters = rows // P_SIZE
    sensors = sensor_cell.shape[0]
    cap = max(2, links // 16)
    groups = 4 if links % 4 == 0 else 1
    per_group = links // groups
    lanes = 1 << (max(ceil_to(4 * cap + links, 128), ceil_to((4 + groups) * clusters, 128)) - 1).bit_length()
    wide = 256 if sensors % 256 == 0 else 128
    dims = dict(
        links=links, rows=rows, clusters=clusters, sensors=sensors, cap=cap, groups=groups, per_group=per_group,
        lanes=lanes, wide=wide, unroll=divisor_up_to(per_group, 12), chunks=3 if cap % 3 == 0 else 1,
        loads=divisor_up_to(links, 8),
    )
    full = (clusters, P_SIZE, S)
    term = (P_SIZE, S)
    chunks, pieces = dims["chunks"], sensors // wide

    def as_row(x):
        return jnp.pad(x.reshape(1, links), ((0, 0), (0, lanes - links)))

    vmem = pl.BlockSpec(memory_space=pltpu.VMEM)
    hbm = pl.BlockSpec(memory_space=pl.ANY)
    dma = pltpu.SemaphoreType.DMA
    scratch = [
        pltpu.VMEM((links, P_SIZE, P_SIZE), jnp.bfloat16),
        pltpu.VMEM(full, jnp.bfloat16),
        pltpu.VMEM(full, jnp.bfloat16),
        pltpu.VMEM(full, jnp.float32),
        pltpu.VMEM((rows, S), jnp.float32),
        pltpu.VMEM(full, jnp.float32),
        pltpu.VMEM((per_group + 1, *term), jnp.float32),
        pltpu.VMEM((4, cap + 1, *term), jnp.float32),
        pltpu.VMEM((SWEEPS, 4 * cap, *term), jnp.bfloat16),
        pltpu.VMEM((SWEEPS, 4 * cap, *term), jnp.bfloat16),
        pltpu.VMEM((3, TAPS, sensors), jnp.int32),
        pltpu.VMEM((3, TAPS, sensors), jnp.float32),
        pltpu.VMEM((2, TAPS, sensors), jnp.int32),
        pltpu.VMEM((2, TAPS, sensors), jnp.float32),
        pltpu.VMEM((3 * pieces, rows, wide), jnp.bfloat16),
        pltpu.VMEM((S, rows), jnp.bfloat16),
        pltpu.VMEM((2, pieces, S, wide), jnp.bfloat16),
        pltpu.VMEM((2, pieces, S, wide), jnp.bfloat16),
        pltpu.VMEM((pieces, S, wide), jnp.float32),
        pltpu.VMEM((8, lanes), jnp.int32),
        pltpu.VMEM((4, 8, lanes), jnp.int32),
        pltpu.SMEM((8, lanes), jnp.int32),
        pltpu.SMEM((4, 8, lanes), jnp.int32),
        dma((dims["loads"] + 2,)),
        dma((2,)),
        dma((3, 4)),
        dma((3, 4)),
        dma((SWEEPS, 4, chunks)),
        dma((SWEEPS, 4, chunks)),
        dma((2, pieces)),
        dma((2, pieces)),
    ]
    radiosity, values = pl.pallas_call(
        functools.partial(fused_kernel, dims=dims),
        out_shape=[jax.ShapeDtypeStruct(full, jnp.float32), jax.ShapeDtypeStruct((sensors, S), jnp.float32)],
        in_specs=[vmem] * 6 + [hbm] * 2,
        out_specs=[hbm, vmem],
        scratch_shapes=scratch,
        compiler_params=pltpu.CompilerParams(collective_id=0, has_side_effects=True, vmem_limit_bytes=62 * 2**20),
        name="radiosity",
    )(
        as_row(link_target[:, 0]),
        as_row(link_slot),
        as_row(link_source),
        sensor_cell.T,
        sensor_weight.T,
        reflectance.reshape(rows // 128, 128),
        emission.reshape(full),
        link_blocks,
    )
    return radiosity.reshape(rows, S), values


def solution(mesh):
    both = ("gx", "gy")
    return jax.shard_map(
        per_device,
        mesh=mesh,
        in_specs=(
            P(both, None),
            P(both),
            P(both, None, None),
            P(both),
            P(both, None),
            P(both),
            P(both, None),
            P(both, None),
        ),
        out_specs=(P(both, None), P(both, None)),
        check_vma=False,
    )
```

```python
import functools

import jax
import jax.numpy as jnp
from jax import lax
from jax.experimental import pallas as pl
from jax.experimental.pallas import tpu as pltpu
from jax.sharding import PartitionSpec as P

P_SIZE = 256
S = 128
SWEEPS = 2
TAPS = 8
MESH = pl.DeviceIdType.MESH
MOVES = (("gy", 1), ("gy", -1), ("gx", 1), ("gx", -1))


def ceil_to(n, m):
    return -(-n // m) * m


def divisor_up_to(n, most):
    return max(d for d in range(1, most + 1) if n % d == 0)


def turned(row, size):
    return jnp.transpose(jnp.broadcast_to(row, (size, row.shape[1])))


def make_tables(target, slot, source, me, cols, dims):
    links, clusters, cap, per_group, groups, lanes = (
        dims["links"], dims["clusters"], dims["cap"], dims["per_group"], dims["groups"], dims["lanes"],
    )
    lane = lax.broadcasted_iota(jnp.int32, (1, lanes), 1)
    ways = 4 * cap
    away = target - me
    group = jnp.where(
        away == 0, 4, jnp.where(away == cols, 2, jnp.where(away == -cols, 3, jnp.where(away == 1, 0, 1)))
    )
    group = jnp.where(lane < links, group, 5)
    base = group * (clusters * lanes)
    key = base + slot * lanes + lane
    key_m = turned(key, lanes)
    rank = jnp.sum(jnp.where((key_m < key) & (key_m >= base), 1, 0), axis=0, keepdims=True)
    place = jnp.where(group == 4, ways + rank, group * cap + rank)
    place = jnp.where(lane < links, place, -1)
    code = lane + lanes * (source + 64 * (slot + 64))
    place_m, code_m = turned(place, lanes), turned(code, lanes)
    wide = lax.broadcasted_iota(jnp.int32, (lanes, lanes), 1)
    found = jnp.sum(jnp.where(place_m == wide, code_m, 0), axis=0, keepdims=True)
    block = found & (lanes - 1)
    rest = found >> (lanes.bit_length() - 1)
    from_cluster = rest & 63
    into = jnp.where(rest >= 4096, (rest >> 6) & 63, -1)
    starts = [w * cap for w in range(4)] + [ways + g * per_group for g in range(groups)]
    ends = starts[1:] + [ways + groups * per_group]
    keep = into == pltpu.roll(jnp.broadcast_to(into, (8, lanes)), 1, 1)[0:1]
    for start in starts:
        keep = keep & (lane != start)
    keep = jnp.where(keep & (into >= 0), 1, 0)
    into_m = turned(into, lanes)
    order = lax.broadcasted_iota(jnp.int32, (lanes, lanes), 0)
    first = jnp.zeros((1, lanes), jnp.int32)
    end = jnp.zeros((1, lanes), jnp.int32)
    cluster = jnp.full((1, lanes), -2, jnp.int32)
    for g in range(4 + groups):
        inside = (lane >= g * clusters) & (lane < (g + 1) * clusters)
        first = jnp.where(inside, starts[g], first)
        end = jnp.where(inside, ends[g], end)
        cluster = jnp.where(inside, lane - g * clusters, cluster)
    hit = (into_m == cluster) & (order >= first) & (order < end)
    last = jnp.max(jnp.where(hit, order - first + 1, 0), axis=0, keepdims=True)
    row = lax.broadcasted_iota(jnp.int32, (8, lanes), 0)
    return jnp.where(row == 0, block, jnp.where(row == 1, from_cluster, jnp.where(row == 2, keep, last)))


def fused_kernel(
    target, slot, source, cells, weights, reflect, emission_hbm, blocks_hbm,
    rad_hbm, sum_own,
    blocks, emission, rounded, crossed, rad, refl, acc, running, arrived, sends, recvs, item_cell, item_weight, from_cell,
    from_weight, sensor_w, final_t, sum_send, sum_recv, link_rows, table, table_in, table_s, table_in_s,
    load_sem, table_sem, small_send, small_recv, term_send, term_recv, sum_ssem, sum_rsem,
    *, dims,
):
    clusters, cap, per_group, groups = dims["clusters"], dims["cap"], dims["per_group"], dims["groups"]
    unroll, chunks, loads, sensors = dims["unroll"], dims["chunks"], dims["loads"], dims["sensors"]
    rows, links, lanes = dims["rows"], dims["links"], dims["lanes"]
    ways = 4 * cap
    per_chunk = cap // chunks
    wide = dims["wide"]
    pieces = sensors // wide
    half_rows, half_cols = P_SIZE // 2, S // 2
    i, j = lax.axis_index("gx"), lax.axis_index("gy")
    n_gx, n_gy = lax.axis_size("gx"), lax.axis_size("gy")
    me = i * n_gy + j

    def there(way, back=False):
        axis, step = MOVES[way]
        step = -step if back else step
        at = (j if axis == "gy" else i) + step
        inside = (at >= 0) & (at < (n_gy if axis == "gy" else n_gx))
        return inside, ((i, at) if axis == "gy" else (at, j))

    def remote(src, dst, send, recv, way):
        return pltpu.make_async_remote_copy(
            src_ref=src, dst_ref=dst, send_sem=send, recv_sem=recv, device_id=there(way)[1], device_id_type=MESH
        )

    def if_to(way, act):
        pl.when(there(way)[0])(act)

    def if_from(way, act):
        pl.when(there(way, back=True)[0])(act)

    share = links // loads
    reads = [
        pltpu.make_async_copy(emission_hbm, emission, load_sem.at[loads]),
        pltpu.make_async_copy(emission_hbm, rounded, load_sem.at[loads + 1]),
    ]
    block_reads = [
        pltpu.make_async_copy(blocks_hbm.at[pl.ds(n * share, share)], blocks.at[pl.ds(n * share, share)], load_sem.at[n])
        for n in range(loads)
    ]
    for read in reads + block_reads:
        read.start()

    barrier = pltpu.get_barrier_semaphore()
    for way in range(4):
        if_to(way, lambda way=way: pl.semaphore_signal(barrier, 1, device_id=there(way)[1], device_id_type=MESH))

    link_rows[...] = jnp.zeros(link_rows.shape, jnp.int32)
    for n, link in enumerate((target, slot, source)):
        link_rows[n, :, 0:links] = link[...]
    table[...] = make_tables(link_rows[0], link_rows[1], link_rows[2], me, n_gy, dims)
    table_copy = pltpu.make_async_copy(table, table_s, table_sem.at[0])
    table_copy.start()

    pl.semaphore_wait(barrier, sum(jnp.where(there(way)[0], 1, 0) for way in range(4)))

    def table_send(way):
        return remote(table, table_in.at[way], small_send.at[0, way], small_recv.at[0, way], way)

    def cell_send(way):
        return remote(cells, from_cell.at[way], small_send.at[1, way], small_recv.at[1, way], way)

    def weight_send(way):
        return remote(weights, from_weight.at[way], small_send.at[2, way], small_recv.at[2, way], way)

    for way in range(4):
        if_to(way, lambda way=way: table_send(way).start())
    for way in range(2):
        if_to(way, lambda way=way: cell_send(way).start())
        if_to(way, lambda way=way: weight_send(way).start())

    def spread(t, carry):
        at = pl.ds(pl.multiple_of(t * 128, 128), 128)
        refl[at, :] = turned(reflect[pl.ds(t, 1), :], 128)
        return carry

    lax.fori_loop(0, rows // 128, spread, 0)

    running[0] = jnp.zeros((P_SIZE, S), jnp.float32)
    for way in range(4):
        arrived[way, 0] = jnp.zeros(arrived.shape[2:], jnp.float32)

        @pl.when(jnp.logical_not(there(way, back=True)[0]))
        def _(way=way):
            table_in[way] = jnp.zeros(table_in.shape[1:], jnp.int32)
            if way < 2:
                from_cell[way] = jnp.full(from_cell.shape[1:], -1, jnp.int32)
                from_weight[way] = jnp.zeros(from_weight.shape[1:], jnp.float32)
                sum_recv[way] = jnp.zeros(sum_recv.shape[1:], sum_recv.dtype)

    for read in reads:
        read.wait()

    def cross(c, carry):
        crossed[c] = pltpu.roll(emission[c].astype(jnp.float32), half_cols, 1).astype(jnp.bfloat16)
        return carry

    lax.fori_loop(0, clusters, cross, 0)

    for way in range(4):
        if_from(way, lambda way=way: table_send(way).wait_recv())
    table_in_copy = pltpu.make_async_copy(table_in, table_in_s, table_sem.at[1])
    table_in_copy.start()
    for way in range(2):
        if_from(way, lambda way=way: cell_send(way).wait_recv())
        if_from(way, lambda way=way: weight_send(way).wait_recv())

    for part in range(3):
        cell = cells[...] if part == 2 else from_cell[part]
        weight = weights[...] if part == 2 else from_weight[part]
        total = weight
        for turn in range(1, TAPS):
            total = total + jnp.where(
                cell == pltpu.roll(cell, turn, 0), pltpu.roll(weight, turn, 0), jnp.zeros_like(weight)
            )
        item_cell[part] = cell - (2 * rows, 0, rows)[part]
        item_weight[part] = total

    table_copy.wait()
    table_in_copy.wait()
    for read in block_reads:
        read.wait()

    left = lax.broadcasted_iota(jnp.int32, (half_rows, S), 1) < half_cols

    def term_copy(sweep, half, way, chunk):
        at = pl.ds(way * cap + chunk * per_chunk, per_chunk)
        return remote(
            sends.at[sweep, half, at], recvs.at[sweep, half, at],
            term_send.at[sweep, half, way, chunk], term_recv.at[sweep, half, way, chunk], way,
        )

    def start_terms(sweep, half, pair, chunk):
        for way in pair:
            if_to(way, lambda way=way: term_copy(sweep, half, way, chunk).start())

    def make_terms(sweep, halves, pair):
        def body(chunk, carry):
            for way in pair:
                for r in range(per_chunk):
                    q = way * cap + chunk * per_chunk + r
                    block, cluster = table_s[0, q], table_s[1, q]
                    top = jnp.dot(blocks[block, :half_rows], rounded[cluster], preferred_element_type=jnp.float32)
                    low = jnp.dot(blocks[block, half_rows:], crossed[cluster], preferred_element_type=jnp.float32)
                    for half in halves:
                        packed = jnp.where(left, top, low) if half == 0 else jnp.where(left, low, top)
                        sends[sweep, half, q] = packed.astype(jnp.bfloat16)
            start_terms(sweep, halves[0], pair, chunk)
            return carry

        lax.fori_loop(0, chunks, body, 0)
        for half in halves[1:]:
            for chunk in range(chunks):
                start_terms(sweep, half, pair, chunk)

    def product(q):
        return jnp.dot(blocks[table_s[0, q]], rounded[table_s[1, q]], preferred_element_type=jnp.float32)

    def stay():
        acc[...] = jnp.zeros(acc.shape, jnp.float32)

        def group(g, carry):
            def body(t, carry):
                at = t * unroll
                for u in range(unroll):
                    q = ways + g * per_group + at + u
                    held = jnp.where(table_s[2, q] != 0, running[at + u], 0.0)
                    running[at + u + 1] = product(q) + held
                return carry

            lax.fori_loop(0, per_group // unroll, body, 0)

            def into(c, carry):
                acc[c] += running[table_s[3, (4 + g) * clusters + c]]
                return carry

            lax.fori_loop(0, clusters, into, 0)
            return carry

        lax.fori_loop(0, groups, group, 0)

    def receive(sweep, half, pair):
        def body(chunk, carry):
            for way in pair:
                def scan(way=way):
                    term_copy(sweep, half, way, chunk).wait_recv()
                    for r in range(per_chunk):
                        n = chunk * per_chunk + r
                        held = jnp.where(table_in_s[way, 2, way * cap + n] != 0, arrived[way, n], 0.0)
                        arrived[way, n + 1] = recvs[sweep, half, way * cap + n].astype(jnp.float32) + held

                if_from(way, scan)
            return carry

        lax.fori_loop(0, chunks, body, 0)

    def finish(sweep, half):
        receive(sweep, half, (2, 3))
        receive(sweep, half, (0, 1))
        final = sweep == SWEEPS - 1

        def body(c, carry):
            got = sum(arrived[way, table_in_s[way, 3, way * clusters + c]] for way in range(4))
            for n, came in enumerate((got, pltpu.roll(got, half_cols, 1))):
                part = slice(n * half_rows, (n + 1) * half_rows)
                at = pl.ds(pl.multiple_of(c * P_SIZE + n * half_rows, half_rows), half_rows)
                value = emission[c, part].astype(jnp.float32) + refl[at, :] * (acc[c, part] + came)
                if final:
                    rad[c, part] = value if half == 0 else jnp.where(left, rad[c, part], value)
                    turned_value = jnp.transpose(value)[half * half_cols : (half + 1) * half_cols]
                    final_t[half * half_cols : (half + 1) * half_cols, at] = turned_value.astype(jnp.bfloat16)
                else:
                    if half == 1:
                        value = jnp.where(left, rounded[c, part].astype(jnp.float32), value)
                    rounded[c, part] = value.astype(jnp.bfloat16)
                    crossed[c, part] = pltpu.roll(value, half_cols, 1).astype(jnp.bfloat16)
            return carry

        lax.fori_loop(0, clusters, body, 0)

    tile = 16
    block_rows = 8 * tile
    columns = 3 * sensors // 128
    per_wide = wide // 128

    def sensor_weights(first, end):
        near = lax.broadcasted_iota(jnp.int32, (tile, 128), 0)

        def column(n, carry):
            part = n // (sensors // 128)
            at = pl.ds(pl.multiple_of((n - part * (sensors // 128)) * 128, 128), 128)
            cell = [
                jnp.broadcast_to(item_cell[part, k : k + 1, at], (tile, 128)).astype(jnp.int16) for k in range(TAPS)
            ]
            weight = [
                jnp.broadcast_to(item_weight[part, k : k + 1, at], (tile, 128)).astype(jnp.bfloat16)
                for k in range(TAPS)
            ]
            to = pl.ds(pl.multiple_of((n - (n // per_wide) * per_wide) * 128, 128), 128)

            def body(t, carry):
                for h in range(8):
                    row = pl.multiple_of(t * block_rows + h * tile, tile)
                    here = (near + row).astype(jnp.int16)
                    total = jnp.zeros((tile, 128), jnp.bfloat16)
                    for k in range(TAPS):
                        total = jnp.where(cell[k] == here, weight[k], total)
                    sensor_w[n // per_wide, pl.ds(row, tile), to] = total
                return carry

            lax.fori_loop(0, rows // block_rows, body, 0)
            return carry

        lax.fori_loop(first, end, column, 0)

    def sum_copy(half, way, piece):
        return remote(
            sum_send.at[way, half, piece], sum_recv.at[way, half, piece],
            sum_ssem.at[half, way, piece], sum_rsem.at[half, way, piece], way,
        )

    def sums(half, part, piece):
        mine = final_t[half * half_cols : (half + 1) * half_cols, :]
        return jnp.dot(mine, sensor_w[part * pieces + piece], preferred_element_type=jnp.float32)

    def send_sums(half):
        for piece in range(pieces):
            for part in range(2):
                way = 1 - part
                sum_send[way, half, piece] = sums(half, part, piece).astype(jnp.bfloat16)
                if_to(way, lambda: sum_copy(half, way, piece).start())
        for piece in range(pieces):
            sum_own[piece, half * half_cols : (half + 1) * half_cols] = sums(half, 2, piece)

    def take_sums(half):
        part = slice(half * half_cols, (half + 1) * half_cols)
        for piece in range(pieces):
            for way in range(2):
                if_from(way, lambda: sum_copy(half, way, piece).wait_recv())
            sum_own[piece, part] += sum_recv[0, half, piece].astype(jnp.float32) + sum_recv[1, half, piece].astype(
                jnp.float32
            )

    assert SWEEPS == 2
    make_terms(0, (0, 1), (0, 1))
    make_terms(0, (0, 1), (2, 3))
    stay()
    sensor_weights(0, columns // 4)
    finish(0, 0)
    make_terms(1, (0,), (0, 1))
    make_terms(1, (0,), (2, 3))
    sensor_weights(columns // 4, columns)
    finish(0, 1)
    make_terms(1, (1,), (0, 1))
    make_terms(1, (1,), (2, 3))
    stay()
    finish(1, 0)
    send_sums(0)
    finish(1, 1)
    write = pltpu.make_async_copy(rad, rad_hbm, load_sem.at[0])
    write.start()
    send_sums(1)
    take_sums(0)
    take_sums(1)
    write.wait()

    for way in range(4):
        if_to(way, lambda: table_send(way).wait_send())
        for sweep in range(SWEEPS):
            for half in range(2):
                for chunk in range(chunks):
                    if_to(way, lambda: term_copy(sweep, half, way, chunk).wait_send())
    for way in range(2):
        if_to(way, lambda: cell_send(way).wait_send())
        if_to(way, lambda: weight_send(way).wait_send())
        for half in range(2):
            for piece in range(pieces):
                if_to(way, lambda: sum_copy(half, way, piece).wait_send())


def write_kernel(rad, sums, rad_out, values_out, rad_held, sums_held, values, read_sem, write_sem, *, loads):
    share = rad.shape[0] // loads
    reads = [pltpu.make_async_copy(sums, sums_held, read_sem.at[loads])]
    writes = [pltpu.make_async_copy(values, values_out, write_sem.at[loads])]
    for n in range(loads):
        at = pl.ds(n * share, share)
        reads.append(pltpu.make_async_copy(rad.at[at], rad_held.at[at], read_sem.at[n]))
        writes.append(pltpu.make_async_copy(rad_held.at[at], rad_out.at[at], write_sem.at[n]))
    for read in reads:
        read.start()
    for n, (read, write) in enumerate(zip(reads, writes)):
        read.wait()
        if n == 0:
            wide = sums.shape[2]
            for piece in range(sums.shape[0]):
                values[piece * wide : (piece + 1) * wide, :] = jnp.transpose(sums_held[piece])
        write.start()
    for write in writes:
        write.wait()


def per_device(
    emission,
    reflectance,
    link_blocks,
    link_source,
    link_target,
    link_slot,
    sensor_cell,
    sensor_weight,
):
    links = link_blocks.shape[0]
    rows = emission.shape[0]
    clusters = rows // P_SIZE
    sensors = sensor_cell.shape[0]
    cap = max(2, links // 16)
    groups = 4 if links % 4 == 0 else 1
    per_group = links // groups
    lanes = 1 << (max(ceil_to(4 * cap + links, 128), ceil_to((4 + groups) * clusters, 128)) - 1).bit_length()
    wide = 256 if sensors % 256 == 0 else 128
    dims = dict(
        links=links, rows=rows, clusters=clusters, sensors=sensors, cap=cap, groups=groups, per_group=per_group,
        lanes=lanes, wide=wide, unroll=divisor_up_to(per_group, 12), chunks=3 if cap % 3 == 0 else 1,
        loads=divisor_up_to(links, 8),
    )
    full = (clusters, P_SIZE, S)
    packed = (P_SIZE // 2, S)
    chunks, pieces = dims["chunks"], sensors // wide

    vmem = pl.BlockSpec(memory_space=pltpu.VMEM)
    hbm = pl.BlockSpec(memory_space=pl.ANY)
    dma = pltpu.SemaphoreType.DMA
    scratch = [
        pltpu.VMEM((links, P_SIZE, P_SIZE), jnp.bfloat16),
        pltpu.VMEM(full, jnp.bfloat16),
        pltpu.VMEM(full, jnp.bfloat16),
        pltpu.VMEM(full, jnp.bfloat16),
        pltpu.VMEM(full, jnp.float32),
        pltpu.VMEM((rows, S), jnp.float32),
        pltpu.VMEM(full, jnp.float32),
        pltpu.VMEM((per_group + 1, P_SIZE, S), jnp.float32),
        pltpu.VMEM((4, cap + 1, *packed), jnp.float32),
        pltpu.VMEM((SWEEPS, 2, 4 * cap, *packed), jnp.bfloat16),
        pltpu.VMEM((SWEEPS, 2, 4 * cap, *packed), jnp.bfloat16),
        pltpu.VMEM((3, TAPS, sensors), jnp.int32),
        pltpu.VMEM((3, TAPS, sensors), jnp.float32),
        pltpu.VMEM((2, TAPS, sensors), jnp.int32),
        pltpu.VMEM((2, TAPS, sensors), jnp.float32),
        pltpu.VMEM((3 * pieces, rows, wide), jnp.bfloat16),
        pltpu.VMEM((S, rows), jnp.bfloat16),
        pltpu.VMEM((2, 2, pieces, S // 2, wide), jnp.bfloat16),
        pltpu.VMEM((2, 2, pieces, S // 2, wide), jnp.bfloat16),
        pltpu.VMEM((3, 1, lanes), jnp.int32),
        pltpu.VMEM((8, lanes), jnp.int32),
        pltpu.VMEM((4, 8, lanes), jnp.int32),
        pltpu.SMEM((8, lanes), jnp.int32),
        pltpu.SMEM((4, 8, lanes), jnp.int32),
        dma((dims["loads"] + 2,)),
        dma((2,)),
        dma((3, 4)),
        dma((3, 4)),
        dma((SWEEPS, 2, 4, chunks)),
        dma((SWEEPS, 2, 4, chunks)),
        dma((2, 2, pieces)),
        dma((2, 2, pieces)),
    ]
    radiosity, sums = pl.pallas_call(
        functools.partial(fused_kernel, dims=dims),
        out_shape=[jax.ShapeDtypeStruct(full, jnp.float32), jax.ShapeDtypeStruct((pieces, S, wide), jnp.float32)],
        in_specs=[vmem] * 6 + [hbm] * 2,
        out_specs=[hbm, vmem],
        scratch_shapes=scratch,
        compiler_params=pltpu.CompilerParams(collective_id=0, has_side_effects=True, vmem_limit_bytes=62 * 2**20),
        name="radiosity",
    )(
        link_target[:, 0].reshape(1, links),
        link_slot.reshape(1, links),
        link_source.reshape(1, links),
        sensor_cell.T,
        sensor_weight.T,
        reflectance.reshape(rows // 128, 128),
        emission.reshape(full),
        link_blocks,
    )
    loads = divisor_up_to(clusters, 6)
    radiosity, values = pl.pallas_call(
        functools.partial(write_kernel, loads=loads),
        out_shape=[jax.ShapeDtypeStruct(full, jnp.float32), jax.ShapeDtypeStruct((sensors, S), jnp.float32)],
        in_specs=[hbm] * 2,
        out_specs=[hbm] * 2,
        scratch_shapes=[
            pltpu.VMEM(full, jnp.float32),
            pltpu.VMEM((pieces, S, wide), jnp.float32),
            pltpu.VMEM((sensors, S), jnp.float32),
            dma((loads + 1,)),
            dma((loads + 1,)),
        ],
        name="write",
    )(radiosity, sums)
    return radiosity.reshape(rows, S), values


def solution(mesh):
    both = ("gx", "gy")
    return jax.shard_map(
        per_device,
        mesh=mesh,
        in_specs=(
            P(both, None),
            P(both),
            P(both, None, None),
            P(both),
            P(both, None),
            P(both),
            P(both, None),
            P(both, None),
        ),
        out_specs=(P(both, None), P(both, None)),
        check_vma=False,
    )
```

```python
import functools

import jax
import jax.numpy as jnp
from jax import lax
from jax.experimental import pallas as pl
from jax.experimental.pallas import tpu as pltpu
from jax.sharding import PartitionSpec as P

P_SIZE = 256
S = 128
SWEEPS = 2
TAPS = 8
MESH = pl.DeviceIdType.MESH
MOVES = (("gy", 1), ("gy", -1), ("gx", 1), ("gx", -1))


def ceil_to(n, m):
    return -(-n // m) * m


def divisor_up_to(n, most):
    return max(d for d in range(1, most + 1) if n % d == 0)


def turned(row, size):
    return jnp.transpose(jnp.broadcast_to(row, (size, row.shape[1])))


def make_tables(target, slot, source, me, cols, dims):
    links, clusters, cap, per_group, groups, lanes = (
        dims["links"], dims["clusters"], dims["cap"], dims["per_group"], dims["groups"], dims["lanes"],
    )
    lane = lax.broadcasted_iota(jnp.int32, (1, lanes), 1)
    ways = 4 * cap
    away = target - me
    group = jnp.where(
        away == 0, 4, jnp.where(away == cols, 2, jnp.where(away == -cols, 3, jnp.where(away == 1, 0, 1)))
    )
    group = jnp.where(lane < links, group, 5)
    base = group * (clusters * lanes)
    key = base + slot * lanes + lane
    key_m = turned(key, lanes)
    rank = jnp.sum(jnp.where((key_m < key) & (key_m >= base), 1, 0), axis=0, keepdims=True)
    place = jnp.where(group == 4, ways + rank, group * cap + rank)
    place = jnp.where(lane < links, place, -1)
    code = lane + lanes * (source + 64 * (slot + 64))
    place_m, code_m = turned(place, lanes), turned(code, lanes)
    wide = lax.broadcasted_iota(jnp.int32, (lanes, lanes), 1)
    found = jnp.sum(jnp.where(place_m == wide, code_m, 0), axis=0, keepdims=True)
    block = found & (lanes - 1)
    rest = found >> (lanes.bit_length() - 1)
    from_cluster = rest & 63
    into = jnp.where(rest >= 4096, (rest >> 6) & 63, -1)
    starts = [w * cap for w in range(4)] + [ways + g * per_group for g in range(groups)]
    ends = starts[1:] + [ways + groups * per_group]
    keep = into == pltpu.roll(jnp.broadcast_to(into, (8, lanes)), 1, 1)[0:1]
    for start in starts:
        keep = keep & (lane != start)
    keep = jnp.where(keep & (into >= 0), 1, 0)
    into_m = turned(into, lanes)
    order = lax.broadcasted_iota(jnp.int32, (lanes, lanes), 0)
    first = jnp.zeros((1, lanes), jnp.int32)
    end = jnp.zeros((1, lanes), jnp.int32)
    cluster = jnp.full((1, lanes), -2, jnp.int32)
    for g in range(4 + groups):
        inside = (lane >= g * clusters) & (lane < (g + 1) * clusters)
        first = jnp.where(inside, starts[g], first)
        end = jnp.where(inside, ends[g], end)
        cluster = jnp.where(inside, lane - g * clusters, cluster)
    hit = (into_m == cluster) & (order >= first) & (order < end)
    last = jnp.max(jnp.where(hit, order - first + 1, 0), axis=0, keepdims=True)
    row = lax.broadcasted_iota(jnp.int32, (8, lanes), 0)
    return jnp.where(row == 0, block, jnp.where(row == 1, from_cluster, jnp.where(row == 2, keep, last)))


def fused_kernel(
    target, slot, source, cells, weights, reflect, emission_hbm, blocks_hbm,
    rad_hbm, sum_own,
    blocks, emission, rounded, crossed, rad, refl, acc, running, arrived, sends, recvs, item_cell, item_weight, from_cell,
    from_weight, sensor_w, final_t, sum_send, sum_recv, link_rows, table, table_in, table_s, table_in_s,
    load_sem, table_sem, small_send, small_recv, term_send, term_recv, sum_ssem, sum_rsem,
    passing, hop_send, hop_recv, pass_send,
    *, dims,
):
    clusters, cap, per_group, groups = dims["clusters"], dims["cap"], dims["per_group"], dims["groups"]
    unroll, chunks, loads, sensors = dims["unroll"], dims["chunks"], dims["loads"], dims["sensors"]
    rows, links, lanes = dims["rows"], dims["links"], dims["lanes"]
    ways = 4 * cap
    per_chunk = cap // chunks
    wide = dims["wide"]
    pieces = sensors // wide
    half_rows, half_cols = P_SIZE // 2, S // 2
    i, j = lax.axis_index("gx"), lax.axis_index("gy")
    n_gx, n_gy = lax.axis_size("gx"), lax.axis_size("gy")
    me = i * n_gy + j

    def there(way, back=False):
        axis, step = MOVES[way]
        step = -step if back else step
        at = (j if axis == "gy" else i) + step
        inside = (at >= 0) & (at < (n_gy if axis == "gy" else n_gx))
        return inside, ((i, at) if axis == "gy" else (at, j))

    def remote(src, dst, send, recv, way):
        return pltpu.make_async_remote_copy(
            src_ref=src, dst_ref=dst, send_sem=send, recv_sem=recv, device_id=there(way)[1], device_id_type=MESH
        )

    def if_to(way, act):
        pl.when(there(way)[0])(act)

    def if_from(way, act):
        pl.when(there(way, back=True)[0])(act)

    share = links // loads
    reads = [
        pltpu.make_async_copy(emission_hbm, emission, load_sem.at[loads]),
        pltpu.make_async_copy(emission_hbm, rounded, load_sem.at[loads + 1]),
    ]
    block_reads = [
        pltpu.make_async_copy(blocks_hbm.at[pl.ds(n * share, share)], blocks.at[pl.ds(n * share, share)], load_sem.at[n])
        for n in range(loads)
    ]
    for read in reads + block_reads:
        read.start()

    barrier = pltpu.get_barrier_semaphore()
    for way in range(4):
        if_to(way, lambda way=way: pl.semaphore_signal(barrier, 1, device_id=there(way)[1], device_id_type=MESH))
    for two in (-2, 2):
        pl.when((j + two >= 0) & (j + two < n_gy))(
            lambda two=two: pl.semaphore_signal(barrier, 1, device_id=(i, j + two), device_id_type=MESH)
        )

    link_rows[...] = jnp.zeros(link_rows.shape, jnp.int32)
    for n, link in enumerate((target, slot, source)):
        link_rows[n, :, 0:links] = link[...]
    table[...] = make_tables(link_rows[0], link_rows[1], link_rows[2], me, n_gy, dims)
    table_copy = pltpu.make_async_copy(table, table_s, table_sem.at[0])
    table_copy.start()

    further = jnp.where(j >= 2, 1, 0) + jnp.where(j + 2 < n_gy, 1, 0)
    pl.semaphore_wait(barrier, further + sum(jnp.where(there(way)[0], 1, 0) for way in range(4)))

    def table_send(way):
        return remote(table, table_in.at[way], small_send.at[0, way], small_recv.at[0, way], way)

    def cell_send(way):
        return remote(cells, from_cell.at[way], small_send.at[1, way], small_recv.at[1, way], way)

    def weight_send(way):
        return remote(weights, from_weight.at[way], small_send.at[2, way], small_recv.at[2, way], way)

    for way in range(4):
        if_to(way, lambda way=way: table_send(way).start())
    for way in range(2):
        if_to(way, lambda way=way: cell_send(way).start())
        if_to(way, lambda way=way: weight_send(way).start())

    def spread(t, carry):
        at = pl.ds(pl.multiple_of(t * 128, 128), 128)
        refl[at, :] = turned(reflect[pl.ds(t, 1), :], 128)
        return carry

    lax.fori_loop(0, rows // 128, spread, 0)

    running[0] = jnp.zeros((P_SIZE, S), jnp.float32)
    for way in range(4):
        arrived[way, 0] = jnp.zeros(arrived.shape[2:], jnp.float32)

        @pl.when(jnp.logical_not(there(way, back=True)[0]))
        def _(way=way):
            table_in[way] = jnp.zeros(table_in.shape[1:], jnp.int32)
            if way < 2:
                from_cell[way] = jnp.full(from_cell.shape[1:], -1, jnp.int32)
                from_weight[way] = jnp.zeros(from_weight.shape[1:], jnp.float32)
                sum_recv[way] = jnp.zeros(sum_recv.shape[1:], sum_recv.dtype)

    for read in reads:
        read.wait()

    def cross(c, carry):
        crossed[c] = pltpu.roll(emission[c].astype(jnp.float32), half_cols, 1).astype(jnp.bfloat16)
        return carry

    lax.fori_loop(0, clusters, cross, 0)

    for way in range(4):
        if_from(way, lambda way=way: table_send(way).wait_recv())
    table_in_copy = pltpu.make_async_copy(table_in, table_in_s, table_sem.at[1])
    table_in_copy.start()
    for way in range(2):
        if_from(way, lambda way=way: cell_send(way).wait_recv())
        if_from(way, lambda way=way: weight_send(way).wait_recv())

    for part in range(3):
        cell = cells[...] if part == 2 else from_cell[part]
        weight = weights[...] if part == 2 else from_weight[part]
        total = weight
        for turn in range(1, TAPS):
            total = total + jnp.where(
                cell == pltpu.roll(cell, turn, 0), pltpu.roll(weight, turn, 0), jnp.zeros_like(weight)
            )
        item_cell[part] = cell - (2 * rows, 0, rows)[part]
        item_weight[part] = total

    table_copy.wait()
    table_in_copy.wait()
    for read in block_reads:
        read.wait()

    left = lax.broadcasted_iota(jnp.int32, (half_rows, S), 1) < half_cols

    levels = n_gy // 2 if n_gy % 2 == 0 else 1
    odd = j % 2
    level, mirrored = j // 2, levels - 1 - j // 2
    depth, passed_depth = jnp.where(odd == 1, level, mirrored), jnp.where(odd == 1, mirrored, level)
    via = jnp.where(depth < levels - 1, (levels - 1 - depth) * cap // levels, 0)
    passed = jnp.where(passed_depth < levels - 1, (levels - 1 - passed_depth) * cap // levels, 0)
    cross_way = 1 - odd

    def term_copy(sweep, half, way, n):
        return remote(
            sends.at[sweep, half, way * cap + n], recvs.at[sweep, half, way * cap + n],
            term_send.at[sweep, half, way, n], term_recv.at[sweep, half, way, n], way,
        )

    def hop_copy(sweep, half, n):
        return pltpu.make_async_remote_copy(
            src_ref=sends.at[sweep, half, cross_way * cap + n], dst_ref=passing.at[sweep, half, n],
            send_sem=hop_send.at[sweep, half, n], recv_sem=hop_recv.at[sweep, half, n],
            device_id=(i, j + 1 - 2 * odd), device_id_type=MESH,
        )

    def pass_copy(sweep, half, n):
        return pltpu.make_async_remote_copy(
            src_ref=passing.at[sweep, half, n], dst_ref=recvs.at[sweep, half, odd * cap + n],
            send_sem=pass_send.at[sweep, half, n], recv_sem=term_recv.at[sweep, half, odd, n],
            device_id=(i, j + 2 - 4 * odd), device_id_type=MESH,
        )

    def direct(way, n):
        goes = there(way)[0]
        return goes if way > 1 else goes & jnp.logical_not((cross_way == way) & (n < via))

    def start_direct(sweep, half, way, n):
        pl.when(direct(way, n))(lambda: term_copy(sweep, half, way, n).start())

    def start_via(sweep, half, n):
        pl.when(n < via)(lambda: hop_copy(sweep, half, n).start())

    def each_term(act):
        def body(n, carry):
            act(n)
            return carry

        lax.fori_loop(0, cap, body, 0)

    def pass_on(sweep, half):
        def act(n):
            @pl.when(n < passed)
            def _():
                hop_copy(sweep, half, n).wait_recv()
                pass_copy(sweep, half, n).start()

        each_term(act)

    def make_terms(sweep, halves, pair):
        def body(chunk, carry):
            for way in pair:
                for r in range(per_chunk):
                    q = way * cap + chunk * per_chunk + r
                    block, cluster = table_s[0, q], table_s[1, q]
                    top = jnp.dot(blocks[block, :half_rows], rounded[cluster], preferred_element_type=jnp.float32)
                    low = jnp.dot(blocks[block, half_rows:], crossed[cluster], preferred_element_type=jnp.float32)
                    for half in halves:
                        packed = jnp.where(left, top, low) if half == 0 else jnp.where(left, low, top)
                        sends[sweep, half, q] = packed.astype(jnp.bfloat16)
            for r in range(per_chunk):
                n = chunk * per_chunk + r
                if pair == (0, 1):
                    start_via(sweep, halves[0], n)
                for way in pair:
                    start_direct(sweep, halves[0], way, n)
            return carry

        lax.fori_loop(0, chunks, body, 0)
        for half in halves[1:]:
            if pair == (0, 1):
                each_term(lambda n: start_via(sweep, half, n))
            each_term(lambda n: [start_direct(sweep, half, way, n) for way in pair])

    def product(q):
        return jnp.dot(blocks[table_s[0, q]], rounded[table_s[1, q]], preferred_element_type=jnp.float32)

    def stay(begin, end):
        if begin == 0:
            acc[...] = jnp.zeros(acc.shape, jnp.float32)

        def group(g, carry):
            def body(t, carry):
                at = t * unroll
                for u in range(unroll):
                    q = ways + g * per_group + at + u
                    held = jnp.where(table_s[2, q] != 0, running[at + u], 0.0)
                    running[at + u + 1] = product(q) + held
                return carry

            lax.fori_loop(0, per_group // unroll, body, 0)

            def into(c, carry):
                acc[c] += running[table_s[3, (4 + g) * clusters + c]]
                return carry

            lax.fori_loop(0, clusters, into, 0)
            return carry

        lax.fori_loop(begin, end, group, 0)

    def receive(sweep, half, pair):
        def body(chunk, carry):
            for way in pair:
                def scan(way=way):
                    for r in range(per_chunk):
                        n = chunk * per_chunk + r
                        term_copy(sweep, half, way, n).wait_recv()
                        held = jnp.where(table_in_s[way, 2, way * cap + n] != 0, arrived[way, n], 0.0)
                        arrived[way, n + 1] = recvs[sweep, half, way * cap + n].astype(jnp.float32) + held

                if_from(way, scan)
            return carry

        lax.fori_loop(0, chunks, body, 0)

    def finish(sweep, half):
        receive(sweep, half, (2, 3))
        receive(sweep, half, (0, 1))
        final = sweep == SWEEPS - 1

        step = dims["step"]

        def one(c):
            got = sum(arrived[way, table_in_s[way, 3, way * clusters + c]] for way in range(4))
            for n, came in enumerate((got, pltpu.roll(got, half_cols, 1))):
                part = slice(n * half_rows, (n + 1) * half_rows)
                at = pl.ds(pl.multiple_of(c * P_SIZE + n * half_rows, half_rows), half_rows)
                value = emission[c, part].astype(jnp.float32) + refl[at, :] * (acc[c, part] + came)
                if final:
                    rad[c, part] = value if half == 0 else jnp.where(left, rad[c, part], value)
                    turned_value = jnp.transpose(value)[half * half_cols : (half + 1) * half_cols]
                    final_t[half * half_cols : (half + 1) * half_cols, at] = turned_value.astype(jnp.bfloat16)
                else:
                    if half == 1:
                        value = jnp.where(left, rounded[c, part].astype(jnp.float32), value)
                    rounded[c, part] = value.astype(jnp.bfloat16)
                    crossed[c, part] = pltpu.roll(value, half_cols, 1).astype(jnp.bfloat16)

        def body(t, carry):
            for u in range(step):
                one(t * step + u)
            return carry

        lax.fori_loop(0, clusters // step, body, 0)

    tile = 16
    block_rows = 8 * tile
    columns = 3 * sensors // 128
    per_wide = wide // 128

    def sensor_weights(first, end):
        near = lax.broadcasted_iota(jnp.int32, (tile, 128), 0)

        def column(n, carry):
            part = n // (sensors // 128)
            at = pl.ds(pl.multiple_of((n - part * (sensors // 128)) * 128, 128), 128)
            cell = [
                jnp.broadcast_to(item_cell[part, k : k + 1, at], (tile, 128)).astype(jnp.int16) for k in range(TAPS)
            ]
            weight = [
                jnp.broadcast_to(item_weight[part, k : k + 1, at], (tile, 128)).astype(jnp.bfloat16)
                for k in range(TAPS)
            ]
            to = pl.ds(pl.multiple_of((n - (n // per_wide) * per_wide) * 128, 128), 128)

            def body(t, carry):
                for h in range(8):
                    row = pl.multiple_of(t * block_rows + h * tile, tile)
                    here = (near + row).astype(jnp.int16)
                    total = jnp.zeros((tile, 128), jnp.bfloat16)
                    for k in range(TAPS):
                        total = jnp.where(cell[k] == here, weight[k], total)
                    sensor_w[n // per_wide, pl.ds(row, tile), to] = total
                return carry

            lax.fori_loop(0, rows // block_rows, body, 0)
            return carry

        lax.fori_loop(first, end, column, 0)

    def sum_copy(half, way, piece):
        return remote(
            sum_send.at[way, half, piece], sum_recv.at[way, half, piece],
            sum_ssem.at[half, way, piece], sum_rsem.at[half, way, piece], way,
        )

    def sums(half, part, piece):
        mine = final_t[half * half_cols : (half + 1) * half_cols, :]
        return jnp.dot(mine, sensor_w[part * pieces + piece], preferred_element_type=jnp.float32)

    def send_sums(half):
        for piece in range(pieces):
            for part in range(2):
                way = 1 - part
                sum_send[way, half, piece] = sums(half, part, piece).astype(jnp.bfloat16)
                if_to(way, lambda: sum_copy(half, way, piece).start())
        for piece in range(pieces):
            sum_own[piece, half * half_cols : (half + 1) * half_cols] = sums(half, 2, piece)

    def take_sums(half):
        part = slice(half * half_cols, (half + 1) * half_cols)
        for piece in range(pieces):
            for way in range(2):
                if_from(way, lambda: sum_copy(half, way, piece).wait_recv())
            sum_own[piece, part] += sum_recv[0, half, piece].astype(jnp.float32) + sum_recv[1, half, piece].astype(
                jnp.float32
            )

    assert SWEEPS == 2
    early = groups // 2
    make_terms(0, (0, 1), (0, 1))
    make_terms(0, (0, 1), (2, 3))
    stay(0, early)
    pass_on(0, 0)
    stay(early, groups)
    sensor_weights(0, columns // 4)
    finish(0, 0)
    make_terms(1, (0,), (0, 1))
    make_terms(1, (0,), (2, 3))
    pass_on(0, 1)
    sensor_weights(columns // 4, columns)
    finish(0, 1)
    make_terms(1, (1,), (0, 1))
    make_terms(1, (1,), (2, 3))
    pass_on(1, 0)
    stay(0, groups)
    finish(1, 0)
    pass_on(1, 1)
    send_sums(0)
    finish(1, 1)
    write = pltpu.make_async_copy(rad, rad_hbm, load_sem.at[0])
    write.start()
    send_sums(1)
    take_sums(0)
    take_sums(1)
    write.wait()

    for sweep in range(SWEEPS):
        for half in range(2):
            def close(n):
                for way in range(4):
                    pl.when(direct(way, n))(lambda: term_copy(sweep, half, way, n).wait_send())
                pl.when(n < via)(lambda: hop_copy(sweep, half, n).wait_send())
                pl.when(n < passed)(lambda: pass_copy(sweep, half, n).wait_send())

            each_term(close)
    for way in range(4):
        if_to(way, lambda: table_send(way).wait_send())
    for way in range(2):
        if_to(way, lambda: cell_send(way).wait_send())
        if_to(way, lambda: weight_send(way).wait_send())
        for half in range(2):
            for piece in range(pieces):
                if_to(way, lambda: sum_copy(half, way, piece).wait_send())


def write_kernel(rad, sums, rad_out, values_out, rad_held, sums_held, values, read_sem, write_sem, *, loads):
    share = rad.shape[0] // loads
    reads = [pltpu.make_async_copy(sums, sums_held, read_sem.at[loads])]
    writes = [pltpu.make_async_copy(values, values_out, write_sem.at[loads])]
    for n in range(loads):
        at = pl.ds(n * share, share)
        reads.append(pltpu.make_async_copy(rad.at[at], rad_held.at[at], read_sem.at[n]))
        writes.append(pltpu.make_async_copy(rad_held.at[at], rad_out.at[at], write_sem.at[n]))
    for read in reads:
        read.start()
    for n, (read, write) in enumerate(zip(reads, writes)):
        read.wait()
        if n == 0:
            wide = sums.shape[2]
            for piece in range(sums.shape[0]):
                values[piece * wide : (piece + 1) * wide, :] = jnp.transpose(sums_held[piece])
        write.start()
    for write in writes:
        write.wait()


def per_device(
    emission,
    reflectance,
    link_blocks,
    link_source,
    link_target,
    link_slot,
    sensor_cell,
    sensor_weight,
):
    links = link_blocks.shape[0]
    rows = emission.shape[0]
    clusters = rows // P_SIZE
    sensors = sensor_cell.shape[0]
    cap = max(2, links // 16)
    groups = 4 if links % 4 == 0 else 1
    per_group = links // groups
    lanes = 1 << (max(ceil_to(4 * cap + links, 128), ceil_to((4 + groups) * clusters, 128)) - 1).bit_length()
    wide = 256 if sensors % 256 == 0 else 128
    dims = dict(
        links=links, rows=rows, clusters=clusters, sensors=sensors, cap=cap, groups=groups, per_group=per_group,
        lanes=lanes, wide=wide, unroll=divisor_up_to(per_group, 12), chunks=3 if cap % 3 == 0 else 1,
        loads=divisor_up_to(links, 8), step=divisor_up_to(clusters, 3),
    )
    full = (clusters, P_SIZE, S)
    packed = (P_SIZE // 2, S)
    pieces = sensors // wide

    vmem = pl.BlockSpec(memory_space=pltpu.VMEM)
    hbm = pl.BlockSpec(memory_space=pl.ANY)
    dma = pltpu.SemaphoreType.DMA
    scratch = [
        pltpu.VMEM((links, P_SIZE, P_SIZE), jnp.bfloat16),
        pltpu.VMEM(full, jnp.bfloat16),
        pltpu.VMEM(full, jnp.bfloat16),
        pltpu.VMEM(full, jnp.bfloat16),
        pltpu.VMEM(full, jnp.float32),
        pltpu.VMEM((rows, S), jnp.float32),
        pltpu.VMEM(full, jnp.float32),
        pltpu.VMEM((per_group + 1, P_SIZE, S), jnp.float32),
        pltpu.VMEM((4, cap + 1, *packed), jnp.float32),
        pltpu.VMEM((SWEEPS, 2, 4 * cap, *packed), jnp.bfloat16),
        pltpu.VMEM((SWEEPS, 2, 4 * cap, *packed), jnp.bfloat16),
        pltpu.VMEM((3, TAPS, sensors), jnp.int32),
        pltpu.VMEM((3, TAPS, sensors), jnp.float32),
        pltpu.VMEM((2, TAPS, sensors), jnp.int32),
        pltpu.VMEM((2, TAPS, sensors), jnp.float32),
        pltpu.VMEM((3 * pieces, rows, wide), jnp.bfloat16),
        pltpu.VMEM((S, rows), jnp.bfloat16),
        pltpu.VMEM((2, 2, pieces, S // 2, wide), jnp.bfloat16),
        pltpu.VMEM((2, 2, pieces, S // 2, wide), jnp.bfloat16),
        pltpu.VMEM((3, 1, lanes), jnp.int32),
        pltpu.VMEM((8, lanes), jnp.int32),
        pltpu.VMEM((4, 8, lanes), jnp.int32),
        pltpu.SMEM((8, lanes), jnp.int32),
        pltpu.SMEM((4, 8, lanes), jnp.int32),
        dma((dims["loads"] + 2,)),
        dma((2,)),
        dma((3, 4)),
        dma((3, 4)),
        dma((SWEEPS, 2, 4, cap)),
        dma((SWEEPS, 2, 4, cap)),
        dma((2, 2, pieces)),
        dma((2, 2, pieces)),
        pltpu.VMEM((SWEEPS, 2, cap, *packed), jnp.bfloat16),
        dma((SWEEPS, 2, cap)),
        dma((SWEEPS, 2, cap)),
        dma((SWEEPS, 2, cap)),
    ]
    radiosity, sums = pl.pallas_call(
        functools.partial(fused_kernel, dims=dims),
        out_shape=[jax.ShapeDtypeStruct(full, jnp.float32), jax.ShapeDtypeStruct((pieces, S, wide), jnp.float32)],
        in_specs=[vmem] * 6 + [hbm] * 2,
        out_specs=[hbm, vmem],
        scratch_shapes=scratch,
        compiler_params=pltpu.CompilerParams(collective_id=0, has_side_effects=True, vmem_limit_bytes=62 * 2**20),
        name="radiosity",
    )(
        link_target[:, 0].reshape(1, links),
        link_slot.reshape(1, links),
        link_source.reshape(1, links),
        sensor_cell.T,
        sensor_weight.T,
        reflectance.reshape(rows // 128, 128),
        emission.reshape(full),
        link_blocks,
    )
    loads = divisor_up_to(clusters, 6)
    radiosity, values = pl.pallas_call(
        functools.partial(write_kernel, loads=loads),
        out_shape=[jax.ShapeDtypeStruct(full, jnp.float32), jax.ShapeDtypeStruct((sensors, S), jnp.float32)],
        in_specs=[hbm] * 2,
        out_specs=[hbm] * 2,
        scratch_shapes=[
            pltpu.VMEM(full, jnp.float32),
            pltpu.VMEM((pieces, S, wide), jnp.float32),
            pltpu.VMEM((sensors, S), jnp.float32),
            dma((loads + 1,)),
            dma((loads + 1,)),
        ],
        name="write",
    )(radiosity, sums)
    return radiosity.reshape(rows, S), values


def solution(mesh):
    both = ("gx", "gy")
    return jax.shard_map(
        per_device,
        mesh=mesh,
        in_specs=(
            P(both, None),
            P(both),
            P(both, None, None),
            P(both),
            P(both, None),
            P(both),
            P(both, None),
            P(both, None),
        ),
        out_specs=(P(both, None), P(both, None)),
        check_vma=False,
    )
```
